32 devices in a mesh: ops: 8 (over z, y), site: 4 (over x, core).
Axes of the slice: x: 2, y: 2, z: 4, core: 2. Of those that a mesh axis runs over, the one named last changes fastest.
Arguments:
- wavefunction: bfloat16 [2048, 2048], replicated, may hold values from -6 to 6
- left_blocks: bfloat16 [64, 16, 192, 192], P('ops', 'site'), may hold values from -0.4375 to 0.4375
- right_blocks: bfloat16 [64, 16, 192, 192], P('ops', 'site'), may hold values from -0.15625 to 0.15625
- left_sector: int32 [2048], replicated, may hold values from 0 to 15, as said below
- right_sector: int32 [2048], replicated, may hold values from 0 to 15, as said below
- term_count: int32 [8], P('ops'), may hold values from 1 to 8, as said below
- left_energy: float32 [2048], replicated, may hold values from -1 to 1
- right_energy: float32 [2048], replicated, may hold values from -1 to 1
- subspace: bfloat16 [2, 16, 192, 2048], P(None, 'site'), may hold values from -0.0078125 to 0.0078125
Outputs:
- sigma: bfloat16 [16, 192, 2048], P('site')
- projections: float32 [2], replicated
The draws below stay inside these ranges and needn't reach their ends.
Inputs may be any that keep to these rules, and one draw needn't show every extreme that they name: `left_sector`: sector ids never fall along the bond; each of the 16 sectors has 1 to 192 states and one has exactly 192. `right_sector`: sector ids never fall along the bond; each of the 16 sectors has 1 to 192 states and one has exactly 192. `term_count`: some group has all 8 slots live.
All inputs are finite; a program needn't handle non-finite values.
Results may differ from the reference program's by a relative error of at most 0.0045.
Values may be sent and summed in bfloat16 or wider, within the bound.
A program may use at most 192 MiB of HBM per device.

```python
import jax
import jax.numpy as jnp
from jax import lax

M = 2048
NB = 16
MAXB = 192
TERMS_DEV = 8
SUB = 2
TERMS = 64
N_OPS = 8


def draw_term_count(key, part):
    base_counts = jax.random.randint(jax.random.fold_in(key, 11), (N_OPS,), 1, TERMS_DEV // 2 + 1)
    fullest = jax.random.randint(jax.random.fold_in(key, 12), (), 0, N_OPS)
    return jnp.where(jnp.arange(N_OPS) == fullest, TERMS_DEV, base_counts).astype(jnp.int32)


def sector_draw(key):
    biggest = jax.random.randint(jax.random.fold_in(key, 1), (), 0, NB)
    remaining = jnp.int32(M - MAXB)
    sizes = []
    for label in range(NB):
        after = jnp.int32(NB - 1 - label) - (biggest > label).astype(jnp.int32)
        lower = jnp.maximum(1, remaining - after * MAXB)
        upper = jnp.minimum(MAXB, remaining - after)
        picked = jax.random.randint(jax.random.fold_in(key, 100 + label), (), lower, upper + 1)
        is_big = biggest == label
        size_now = jnp.where(is_big, jnp.int32(MAXB), picked).astype(jnp.int32)
        remaining = jnp.where(is_big, remaining, remaining - picked).astype(jnp.int32)
        sizes.append(size_now)
    ends = jnp.cumsum(jnp.stack(sizes)).astype(jnp.int32)
    positions = jnp.arange(M, dtype=jnp.int32)
    return jnp.sum((ends[None, :] <= positions[:, None]).astype(jnp.int32), axis=1).astype(jnp.int32)


def draw_left_sector(key, part):
    return sector_draw(jax.random.fold_in(key, 31))


def draw_right_sector(key, part):
    return sector_draw(jax.random.fold_in(key, 32))


def shard_levels(own_key, shape, shards, low, top_value):
    def one(axis_at, parts):
        heights = jax.random.uniform(jax.random.fold_in(jax.random.fold_in(own_key, 6), axis_at), (parts,), jnp.float32, low / len(shards), top_value / len(shards))
        return jnp.repeat(jnp.exp(heights), shape[axis_at] // parts).reshape((-1,) + (1,) * (len(shape) - axis_at - 1))

    loudness = one(*shards[0])
    for cut in shards[1:]:
        loudness = loudness * one(*cut)
    return loudness


def scatter_about(key, shape, deviation, reach, shards=(), held_as=jnp.bfloat16):
    drawn = deviation * jax.random.normal(key, shape, jnp.float32)
    if shards:
        drawn = drawn * shard_levels(key, shape, shards, -0.22, 0.18)
    return jnp.clip(drawn, -reach, reach).astype(held_as)


def setup_inputs(seed: int = 0) -> dict:
    seeds = jax.random.split(jax.random.key(seed), 10)
    wavefunction = scatter_about(seeds[0], (M, M), 1.0, 6.0)
    left_blocks = scatter_about(seeds[1], (TERMS, NB, MAXB, MAXB), MAXB ** -0.5, 0.4375, ((0, 8), (1, 4)))
    right_blocks = scatter_about(seeds[2], (TERMS, NB, MAXB, MAXB), (MAXB * TERMS_DEV * N_OPS // 8) ** -0.5, 0.15625, ((0, 8), (1, 4)))
    left_sector = draw_left_sector(jax.random.fold_in(seeds[9], 71), 0)
    right_sector = draw_right_sector(jax.random.fold_in(seeds[9], 71), 0)
    term_count = draw_term_count(jax.random.fold_in(seeds[9], 71), 0)
    left_energy = jnp.clip(jax.random.uniform(seeds[6], (M,), jnp.float32, -1.0, 1.0), -1.0, 1.0)
    right_energy = jnp.clip(jax.random.uniform(seeds[7], (M,), jnp.float32, -1.0, 1.0), -1.0, 1.0)
    subspace = scatter_about(seeds[8], (SUB, NB, MAXB, M), (1.0 / M), 0.0078125, ((1, 4),))
    return {"wavefunction": wavefunction, "left_blocks": left_blocks, "right_blocks": right_blocks, "left_sector": left_sector, "right_sector": right_sector, "term_count": term_count, "left_energy": left_energy, "right_energy": right_energy, "subspace": subspace}


def sector_tables(sector_ids, sectors):
    labels = jnp.arange(sectors, dtype=jnp.int32)
    sector_starts = jnp.sum((sector_ids[None, :] < labels[:, None]).astype(jnp.int32), axis=1)
    sector_sizes = jnp.sum((sector_ids[None, :] == labels[:, None]).astype(jnp.int32), axis=1)
    return sector_starts.astype(jnp.int32), sector_sizes.astype(jnp.int32)


def reference(wavefunction, left_blocks, right_blocks, left_sector, right_sector, term_count, left_energy, right_energy, subspace):
    left_start, left_size = sector_tables(left_sector, NB)
    right_start, right_size = sector_tables(right_sector, NB)
    positions = jnp.arange(MAXB, dtype=jnp.int32)
    left_inside = positions[None, :] < left_size[:, None]
    right_inside = positions[None, :] < right_size[:, None]
    left_masks = left_inside[:, :, None] & left_inside[:, None, :]
    right_masks = right_inside[:, :, None] & right_inside[:, None, :]
    psi_padded = jnp.concatenate([wavefunction, jnp.zeros((MAXB, M), wavefunction.dtype)], axis=0)
    psi_slabs = jax.vmap(lambda row_start: lax.dynamic_slice_in_dim(psi_padded, row_start, MAXB, 0))(left_start)
    slab_values = psi_slabs.astype(jnp.float32)
    row_count = NB * MAXB

    def term_product(accum, term_idx):
        live = (term_idx % TERMS_DEV) < term_count[term_idx // TERMS_DEV]

        def apply_term(summed_in):
            blocks = jnp.where(left_masks, left_blocks[term_idx], jnp.zeros((), left_blocks.dtype)).astype(jnp.float32)
            left_image = jnp.einsum("qab,qbc->qac", blocks, slab_values, precision=lax.Precision.HIGHEST)
            rounded = lax.optimization_barrier(left_image.astype(jnp.bfloat16)).astype(jnp.float32)
            rounded = rounded.reshape(row_count, M)
            padded_image = jnp.concatenate([rounded, jnp.zeros((row_count, MAXB), jnp.float32)], axis=1)
            right_terms = jnp.where(right_masks, right_blocks[term_idx], jnp.zeros((), right_blocks.dtype)).astype(jnp.float32)

            def one_sector(sector, summed):
                col_start = right_start[sector]
                window = lax.dynamic_slice_in_dim(padded_image, col_start, MAXB, 1)
                added = jnp.dot(window, right_terms[sector].T, precision=lax.Precision.HIGHEST)
                previous = lax.dynamic_slice_in_dim(summed, col_start, MAXB, 1)
                return lax.dynamic_update_slice_in_dim(summed, previous + added, col_start, 1)

            return lax.fori_loop(0, NB, one_sector, summed_in)

        return lax.cond(live, apply_term, lambda kept: kept, accum), None

    terms_padded, ignored = lax.scan(term_product, jnp.zeros((row_count, M + MAXB), jnp.float32), jnp.arange(TERMS_DEV * N_OPS, dtype=jnp.int32))
    terms = terms_padded[:, :M].reshape(NB, MAXB, M)
    psi_rows = jnp.where(left_inside[:, :, None], slab_values, jnp.float32(0.0))
    energy_padded = jnp.concatenate([left_energy, jnp.zeros((MAXB,), jnp.float32)])
    energy_rows = jax.vmap(lambda row_start: lax.dynamic_slice_in_dim(energy_padded, row_start, MAXB, 0))(left_start)
    sigma_full = terms + (energy_rows[:, :, None] + right_energy[None, None, :]) * psi_rows
    projections = jnp.sum(subspace.astype(jnp.float32) * sigma_full[None], axis=(1, 2, 3))
    return sigma_full.astype(jnp.bfloat16), projections
```

```python
import functools

import jax
import jax.numpy as jnp
from jax import lax
from jax.experimental import pallas as pl
from jax.experimental.pallas import tpu as pltpu
from jax.sharding import PartitionSpec as P

LANE = 128
MESH = pl.DeviceIdType.MESH


def sector_tables(sector_ids, sectors):
    labels = jnp.arange(sectors, dtype=jnp.int32)
    sector_starts = jnp.sum((sector_ids[None, :] < labels[:, None]).astype(jnp.int32), axis=1)
    sector_sizes = jnp.sum((sector_ids[None, :] == labels[:, None]).astype(jnp.int32), axis=1)
    return (sector_starts, sector_sizes)


def round_up(value, step):
    return (value + step - 1) // step * step


def apply_kernel(
    slots, sec_dev, widest, wide, window,
    starts, sizes, left_ref, slab_ref, right_ref, vectors_ref,
    part_ref, corr_ref,
    psi_pad, images, right_pad, summed,
):
    step = pl.program_id(0)
    rows = sec_dev * widest
    bond_dim = part_ref.shape[1]

    @pl.when(step == 0)
    def _():
        summed[...] = jnp.zeros_like(summed)
        right_pad[...] = jnp.zeros_like(right_pad)

    start = starts[step]
    size_now = sizes[step]
    first = pl.multiple_of(start // LANE * LANE, LANE)
    offset = start - first
    place = lax.broadcasted_iota(jnp.int32, (window, wide), 0)
    column = lax.broadcasted_iota(jnp.int32, (window, wide), 1)
    pick = ((place == column + offset) & (column < size_now)).astype(jnp.bfloat16)
    psi_pad[...] = jnp.dot(
        slab_ref[:, pl.ds(first, window)], pick, preferred_element_type=jnp.float32
    ).astype(jnp.bfloat16)
    for slot in range(slots):
        right_pad[0:widest, slot * wide : slot * wide + widest] = right_ref[slot, 0]
    for within in range(sec_dev):
        at = within * widest
        image = jnp.dot(
            left_ref[within], psi_pad[at : at + widest, :], preferred_element_type=jnp.float32
        ).astype(jnp.bfloat16)
        for slot in range(slots):
            images[at : at + widest, slot * wide : (slot + 1) * wide] = image[
                slot * widest : (slot + 1) * widest, :
            ]
    added = lax.dot_general(
        images[...], right_pad[...], (((1,), (1,)), ((), ())), preferred_element_type=jnp.float32
    )
    high = added.astype(jnp.bfloat16)
    low = (added - high.astype(jnp.float32)).astype(jnp.bfloat16)
    back = (((1,), (1,)), ((), ()))
    summed[:, pl.ds(first, window)] += lax.dot_general(
        high, pick, back, preferred_element_type=jnp.float32
    ) + lax.dot_general(low, pick, back, preferred_element_type=jnp.float32)

    @pl.when(step == pl.num_programs(0) - 1)
    def _():
        chunk = 16
        vectors = vectors_ref.shape[0]

        def fold(idx, totals):
            at = pl.multiple_of(idx * chunk, chunk)
            values = summed[pl.ds(at, chunk), 0:bond_dim]
            part_ref[pl.ds(at, chunk), :] = values.astype(jnp.bfloat16)
            new = []
            for k in range(vectors):
                product = vectors_ref[k, pl.ds(at, chunk), :].astype(jnp.float32) * values
                folded = product[0:8] + product[8:16]
                pieces = [folded[:, c : c + LANE] for c in range(0, bond_dim, LANE)]
                while len(pieces) > 1:
                    pieces = [a + b for a, b in zip(pieces[0::2], pieces[1::2])]
                new.append(totals[k] + pieces[0])
            return tuple(new)

        totals = lax.fori_loop(
            0, rows // chunk, fold, tuple(jnp.zeros((8, LANE), jnp.float32) for _ in range(vectors))
        )
        for k in range(vectors):
            corr_ref[k] = totals[k]


def exchange_kernel(
    groups, sites,
    part_ref, psi_ref, left_e_ref, right_e_ref, corr_ref,
    out_ref, corr_out,
    pair_in, sending, outer_in, corr_ops, corr_sites,
    pair_s, pair_r, outer_s, outer_r, gath_s, gath_r, fwd_s, fwd_r, ops_s, ops_r, site_s, site_r,
):
    outer = groups // 2
    me = lax.axis_index("ops")
    here = lax.axis_index("site")
    row = me // 2
    side = me % 2
    peer = row * 2 + 1 - side
    rows, bond_dim = part_ref.shape[1], part_ref.shape[2]
    step = 256

    barrier = pltpu.get_barrier_semaphore()
    for k in range(1, groups):
        pl.semaphore_signal(
            barrier, inc=1, device_id={"ops": lax.rem(me + k, groups)}, device_id_type=MESH
        )
    for k in range(1, sites):
        pl.semaphore_signal(
            barrier, inc=1, device_id={"site": lax.rem(here + k, sites)}, device_id_type=MESH
        )
    pl.semaphore_wait(barrier, groups - 1 + sites - 1)

    def remote(src, dst, send_sem, recv_sem, target):
        return pltpu.make_async_remote_copy(
            src_ref=src, dst_ref=dst, send_sem=send_sem, recv_sem=recv_sem,
            device_id=target, device_id_type=MESH,
        )

    pair = []
    for k in range(outer):
        dest = lax.rem(row + k + 1, outer)
        copy = remote(
            part_ref.at[dest * 2 + 1 - side], pair_in.at[k], pair_s.at[k], pair_r.at[k], {"ops": peer}
        )
        copy.start()
        pair.append(copy)

    corr_copies = []
    for k in range(1, groups):
        copy = remote(
            corr_ref, corr_ops.at[k], ops_s.at[k], ops_r.at[k], {"ops": lax.rem(me + k, groups)}
        )
        copy.start()
        corr_copies.append(copy)
    corr_ops[0] = corr_ref[...]

    sends = []
    for k in range(outer - 1):
        dest = lax.rem(row + k + 1, outer)
        mine = dest * 2 + side
        pair[k].wait_recv()

        def add(c, carry, k=k, mine=mine):
            cols = pl.ds(pl.multiple_of(c * step, step), step)
            sending[k, :, cols] = (
                part_ref[mine, :, cols].astype(jnp.float32) + pair_in[k, :, cols].astype(jnp.float32)
            ).astype(jnp.bfloat16)
            return carry

        lax.fori_loop(0, bond_dim // step, add, 0)
        copy = remote(sending.at[k], outer_in.at[k], outer_s.at[k], outer_r.at[k], {"ops": mine})
        copy.start()
        sends.append(copy)

    pair[outer - 1].wait_recv()
    for copy in sends:
        copy.wait_recv()

    def finish(c, carry):
        cols = pl.ds(pl.multiple_of(c * step, step), step)
        total = part_ref[me, :, cols].astype(jnp.float32) + pair_in[outer - 1, :, cols].astype(
            jnp.float32
        )
        for k in range(outer - 1):
            total = total + outer_in[k, :, cols].astype(jnp.float32)
        total = total + (left_e_ref[...] + right_e_ref[:, cols]) * psi_ref[:, cols].astype(jnp.float32)
        out_ref[me, :, cols] = total.astype(jnp.bfloat16)
        return carry

    lax.fori_loop(0, bond_dim // step, finish, 0)

    gathers = []
    for k in range(outer - 1):
        dest = lax.rem(row + k + 1, outer)
        copy = remote(
            out_ref.at[me], out_ref.at[me], gath_s.at[k], gath_r.at[k], {"ops": dest * 2 + side}
        )
        copy.start()
        gathers.append(copy)
    forwards = [remote(out_ref.at[me], out_ref.at[me], fwd_s.at[outer - 1], fwd_r.at[outer - 1], {"ops": peer})]
    forwards[0].start()

    for copy in corr_copies:
        copy.wait_recv()

    def corr_add(g, total):
        return total + corr_ops[lax.rem(me - g + groups, groups)]

    corr_sites[0] = lax.fori_loop(0, groups, corr_add, jnp.zeros(corr_ref.shape, jnp.float32))
    site_copies = []
    for k in range(1, sites):
        copy = remote(
            corr_sites.at[0], corr_sites.at[k], site_s.at[k], site_r.at[k],
            {"site": lax.rem(here + k, sites)},
        )
        copy.start()
        site_copies.append(copy)

    for k in range(outer - 1):
        source = lax.rem(row - k - 1 + outer, outer)
        slot = source * 2 + side
        remote(
            out_ref.at[slot], out_ref.at[slot], gath_s.at[k], gath_r.at[k], {"ops": peer}
        ).wait_recv()
        copy = remote(out_ref.at[slot], out_ref.at[slot], fwd_s.at[k], fwd_r.at[k], {"ops": peer})
        copy.start()
        forwards.append(copy)

    for copy in site_copies:
        copy.wait_recv()

    def site_add(g, total):
        return total + corr_sites[lax.rem(here - g + sites, sites)]

    corr_out[...] = lax.fori_loop(0, sites, site_add, jnp.zeros(corr_ref.shape, jnp.float32))

    remote(
        out_ref.at[peer], out_ref.at[peer], fwd_s.at[outer - 1], fwd_r.at[outer - 1], {"ops": peer}
    ).wait_recv()
    for k in range(outer - 1):
        source = lax.rem(row - k - 1 + outer, outer)
        slot = source * 2 + 1 - side
        remote(out_ref.at[slot], out_ref.at[slot], fwd_s.at[k], fwd_r.at[k], {"ops": peer}).wait_recv()
    for copy in pair + corr_copies + sends + gathers + forwards + site_copies:
        copy.wait_send()


def local(
    wavefunction,
    left_blocks,
    right_blocks,
    left_sector,
    right_sector,
    term_count,
    left_energy,
    right_energy,
    subspace,
):
    slots, sec_dev, widest = left_blocks.shape[0], left_blocks.shape[1], left_blocks.shape[2]
    bond_dim = wavefunction.shape[0]
    vectors = subspace.shape[0]
    rows = sec_dev * widest
    sites = lax.axis_size("site")
    groups = lax.axis_size("ops")
    sectors = sec_dev * sites
    wide = round_up(widest, 256)
    window = round_up(widest + LANE - 1, LANE)
    padded_cols = round_up(bond_dim, LANE) - LANE + window

    gathered = lax.all_gather(right_blocks, "site", axis=1, tiled=True)

    left_start, left_size = sector_tables(left_sector, sectors)
    right_start, right_size = sector_tables(right_sector, sectors)
    first_sector = lax.axis_index("site") * sec_dev
    psi_padded = jnp.pad(wavefunction, ((0, widest), (0, padded_cols - bond_dim)))
    energy_padded = jnp.pad(left_energy, (0, widest))
    slabs = []
    energies = []
    insides = []
    for within in range(sec_dev):
        row_start = left_start[first_sector + within]
        inside = jnp.arange(widest, dtype=jnp.int32) < left_size[first_sector + within]
        slab = lax.dynamic_slice_in_dim(psi_padded, row_start, widest, 0)
        slabs.append(jnp.where(inside[:, None], slab, jnp.zeros((), slab.dtype)))
        energies.append(lax.dynamic_slice_in_dim(energy_padded, row_start, widest, 0))
        insides.append(inside)
    slab = jnp.concatenate(slabs, axis=0)
    energy = jnp.concatenate(energies)
    inside = jnp.stack(insides)
    live = jnp.arange(slots, dtype=jnp.int32) < term_count[0]
    keep = live[:, None, None, None] & inside[None, :, :, None] & inside[None, :, None, :]
    left = jnp.where(keep, left_blocks, jnp.zeros((), left_blocks.dtype))
    left = left.transpose(1, 0, 2, 3).reshape(sec_dev, slots * widest, widest)
    vectors_flat = subspace.reshape(vectors, rows, bond_dim)

    own = lax.axis_index("ops")
    psi_mine = slab[:, :bond_dim]
    diagonal = (energy[:, None] + right_energy[None, :]) * psi_mine.astype(jnp.float32)
    first_group = jnp.where(own == 0, jnp.float32(1.0), jnp.float32(0.0))
    corr_diag = first_group * jnp.sum(
        vectors_flat.astype(jnp.float32) * diagonal[None], axis=(1, 2)
    )

    vmem = pl.BlockSpec(memory_space=pltpu.VMEM)
    smem = pl.BlockSpec(memory_space=pltpu.SMEM)
    part, corr = pl.pallas_call(
        functools.partial(apply_kernel, slots, sec_dev, widest, wide, window),
        grid=(sectors,),
        out_shape=(
            jax.ShapeDtypeStruct((rows, bond_dim), jnp.bfloat16),
            jax.ShapeDtypeStruct((vectors, 8, LANE), jnp.float32),
        ),
        in_specs=[
            smem,
            smem,
            vmem,
            vmem,
            pl.BlockSpec((slots, 1, widest, widest), lambda step: (0, step, 0, 0)),
            vmem,
        ],
        out_specs=(vmem, vmem),
        scratch_shapes=[
            pltpu.VMEM((rows, wide), jnp.bfloat16),
            pltpu.VMEM((rows, slots * wide), jnp.bfloat16),
            pltpu.VMEM((wide, slots * wide), jnp.bfloat16),
            pltpu.VMEM((rows, padded_cols), jnp.float32),
        ],
        compiler_params=pltpu.CompilerParams(
            dimension_semantics=("arbitrary",), vmem_limit_bytes=60 * 1024 * 1024
        ),
        name="apply_terms",
    )(right_start, right_size, left, slab, gathered, vectors_flat)

    share = rows // groups
    corr_mine = jnp.sum(corr, axis=(1, 2)) + corr_diag
    corr_tile = jnp.broadcast_to(corr_mine[:, None, None], (vectors, 8, LANE))
    psi_share = lax.dynamic_slice_in_dim(psi_mine, own * share, share, 0)
    energy_share = lax.dynamic_slice_in_dim(energy, own * share, share, 0)[:, None]
    outer = groups // 2
    dma = pltpu.SemaphoreType.DMA
    sigma, corr_all = pl.pallas_call(
        functools.partial(exchange_kernel, groups, sites),
        out_shape=(
            jax.ShapeDtypeStruct((groups, share, bond_dim), jnp.bfloat16),
            jax.ShapeDtypeStruct((vectors, 8, LANE), jnp.float32),
        ),
        in_specs=[vmem] * 5,
        out_specs=(vmem, vmem),
        scratch_shapes=[
            pltpu.VMEM((outer, share, bond_dim), jnp.bfloat16),
            pltpu.VMEM((max(outer - 1, 1), share, bond_dim), jnp.bfloat16),
            pltpu.VMEM((max(outer - 1, 1), share, bond_dim), jnp.bfloat16),
            pltpu.VMEM((groups, vectors, 8, LANE), jnp.float32),
            pltpu.VMEM((sites, vectors, 8, LANE), jnp.float32),
            dma((outer,)), dma((outer,)),
            dma((outer,)), dma((outer,)),
            dma((outer,)), dma((outer,)),
            dma((outer,)), dma((outer,)),
            dma((groups,)), dma((groups,)),
            dma((sites,)), dma((sites,)),
        ],
        compiler_params=pltpu.CompilerParams(
            collective_id=0, has_side_effects=True, vmem_limit_bytes=60 * 1024 * 1024
        ),
        name="exchange_rows",
    )(
        part.reshape(groups, share, bond_dim),
        psi_share,
        energy_share,
        right_energy[None, :],
        corr_tile,
    )
    return (sigma.reshape(sec_dev, widest, bond_dim), corr_all[:, 0, 0])


def solution(mesh):
    in_specs = (
        P(),
        P("ops", "site", None, None),
        P("ops", "site", None, None),
        P(),
        P(),
        P("ops"),
        P(),
        P(),
        P(None, "site", None, None),
    )
    out_specs = (P("site", None, None), P())
    return jax.shard_map(local, mesh=mesh, in_specs=in_specs, out_specs=out_specs, check_vma=False)
```

```python
import functools

import jax
import jax.numpy as jnp
from jax import lax
from jax.experimental import pallas as pl
from jax.experimental.pallas import tpu as pltpu
from jax.sharding import PartitionSpec as P

LANE = 128
MESH = pl.DeviceIdType.MESH


def sector_tables(sector_ids, sectors):
    labels = jnp.arange(sectors, dtype=jnp.int32)
    sector_starts = jnp.sum((sector_ids[None, :] < labels[:, None]).astype(jnp.int32), axis=1)
    sector_sizes = jnp.sum((sector_ids[None, :] == labels[:, None]).astype(jnp.int32), axis=1)
    return (sector_starts, sector_sizes)


def round_up(value, step):
    return (value + step - 1) // step * step


def apply_kernel(
    slots, sec_dev, widest, wide,
    left_ref, spread_ref, right_ref,
    out_ref,
    psi_pad, images, right_pad, arrived, added,
    pair_s, pair_r, outer_s, outer_r, fwd_s, fwd_r, out_s,
):
    me = lax.axis_index("site")
    row = me // 2
    side = me % 2
    peer = row * 2 + 1 - side
    across = (1 - row) * 2 + side
    far = (1 - row) * 2 + 1 - side
    pairs = slots // 2
    shift = wide - widest

    barrier = pltpu.get_barrier_semaphore()
    for other in (peer, across):
        pl.semaphore_signal(barrier, inc=1, device_id={"site": other}, device_id_type=MESH)
    pl.semaphore_wait(barrier, 2)

    def to_pair(w):
        return pltpu.make_async_remote_copy(
            src_ref=right_ref.at[w], dst_ref=arrived.at[0, w], send_sem=pair_s.at[w],
            recv_sem=pair_r.at[w], device_id={"site": peer}, device_id_type=MESH,
        )

    def to_across(w):
        return pltpu.make_async_remote_copy(
            src_ref=right_ref.at[w], dst_ref=arrived.at[1, w], send_sem=outer_s.at[w],
            recv_sem=outer_r.at[w], device_id={"site": across}, device_id_type=MESH,
        )

    def forward(w):
        return pltpu.make_async_remote_copy(
            src_ref=arrived.at[1, w], dst_ref=arrived.at[2, w], send_sem=fwd_s.at[w],
            recv_sem=fwd_r.at[w], device_id={"site": peer}, device_id_type=MESH,
        )

    for w in range(sec_dev):
        to_across(w).start()
    for w in range(sec_dev):
        to_pair(w).start()
    right_pad[...] = jnp.zeros_like(right_pad)
    lane_in = lax.broadcasted_iota(jnp.int32, (wide, wide), 0)
    lane_out = lax.broadcasted_iota(jnp.int32, (wide, wide), 1)
    moved = (lane_in + shift == lane_out).astype(jnp.bfloat16)

    def keep(slot, sector):
        return pltpu.make_async_copy(added.at[slot], out_ref.at[sector], out_s.at[slot])

    def one_sector(i, carry):
        @pl.when((i % 3 == 0) & (i > 0) & (i <= 3 * sec_dev))
        def _():
            w = i // 3 - 1
            to_across(w).wait_recv()
            forward(w).start()

        @pl.when(i < sec_dev)
        def _():
            right_pad[0:widest, :] = right_ref[jnp.minimum(i, sec_dev - 1)]

        @pl.when((i >= sec_dev) & (i < 2 * sec_dev))
        def _():
            w = jnp.clip(i - sec_dev, 0, sec_dev - 1)
            to_pair(w).wait_recv()
            right_pad[0:widest, :] = arrived[0, w]

        later = jnp.maximum(i - 2 * sec_dev, 0)
        late_w = later // 2

        @pl.when((i >= 2 * sec_dev) & (i % 2 == 0))
        def _():
            right_pad[0:widest, :] = arrived[1, late_w]

        @pl.when((i >= 2 * sec_dev) & (i % 2 == 1))
        def _():
            forward(late_w).wait_recv()
            right_pad[0:widest, :] = arrived[2, late_w]

        early = i < 2 * sec_dev
        owner = jnp.where(
            early,
            jnp.where(i < sec_dev, me, peer),
            jnp.where(i % 2 == 0, across, far),
        )
        sector = owner * sec_dev + jnp.where(early, i % sec_dev, late_w)
        psi_pad[0] = spread_ref[sector]
        psi_pad[1] = jnp.dot(
            spread_ref[sector], moved, preferred_element_type=jnp.float32
        ).astype(jnp.bfloat16)
        for within in range(sec_dev):
            at = within * widest
            even, odd = (
                jnp.dot(
                    left_ref[within, parity],
                    psi_pad[parity, at : at + widest, :],
                    preferred_element_type=jnp.float32,
                ).astype(jnp.bfloat16)
                for parity in range(2)
            )
            for p in range(pairs):
                rows = slice(p * widest, (p + 1) * widest)
                base = 2 * p * widest
                images[at : at + widest, base : base + LANE] = even[rows, :LANE]
                images[at : at + widest, base + LANE : base + 2 * LANE] = (
                    even[rows, LANE:] + odd[rows, :LANE]
                )
                images[at : at + widest, base + 2 * LANE : base + 3 * LANE] = odd[rows, LANE:]
        slot = i % 2

        @pl.when(i >= 2)
        def _():
            keep(slot, sector).wait()

        added[slot] = lax.dot_general(
            images[...], right_pad[...], (((1,), (1,)), ((), ())), preferred_element_type=jnp.float32
        )
        keep(slot, sector).start()
        return carry

    lax.fori_loop(0, 4 * sec_dev, one_sector, 0)
    for slot in range(2):
        keep(slot, 0).wait()
    for w in range(sec_dev):
        to_pair(w).wait_send()
        to_across(w).wait_send()
        forward(w).wait_send()


def spread_kernel(wide, window, starts, sizes, slab_ref, spread_ref):
    step = pl.program_id(0)
    start = starts[step]
    size_now = sizes[step]
    first = pl.multiple_of(start // LANE * LANE, LANE)
    offset = start - first
    place = lax.broadcasted_iota(jnp.int32, (window, wide), 0)
    column = lax.broadcasted_iota(jnp.int32, (window, wide), 1)
    pick = ((place == column + offset) & (column < size_now)).astype(jnp.bfloat16)
    spread_ref[0] = jnp.dot(
        slab_ref[:, pl.ds(first, window)], pick, preferred_element_type=jnp.float32
    ).astype(jnp.bfloat16)


def place_kernel(
    widest, wide, window, starts, sizes, added_ref, vectors_ref, part_ref, corr_ref, summed
):
    step = pl.program_id(0)
    rows, bond_dim = part_ref.shape

    @pl.when(step == 0)
    def _():
        summed[...] = jnp.zeros_like(summed)

    start = starts[step]
    size_now = sizes[step]
    first = pl.multiple_of(start // LANE * LANE, LANE)
    offset = start - first
    place = lax.broadcasted_iota(jnp.int32, (window, wide), 0)
    column = lax.broadcasted_iota(jnp.int32, (window, wide), 1)
    pick = ((place == column + offset) & (column < size_now)).astype(jnp.bfloat16)
    added = added_ref[0]
    high = added.astype(jnp.bfloat16)
    low = (added - high.astype(jnp.float32)).astype(jnp.bfloat16)
    back = (((1,), (1,)), ((), ()))
    summed[:, pl.ds(first, window)] += lax.dot_general(
        high, pick, back, preferred_element_type=jnp.float32
    ) + lax.dot_general(low, pick, back, preferred_element_type=jnp.float32)

    @pl.when(step == pl.num_programs(0) - 1)
    def _():
        chunk = 16
        vectors = vectors_ref.shape[0]

        def fold(idx, totals):
            at = pl.multiple_of(idx * chunk, chunk)
            values = summed[pl.ds(at, chunk), 0:bond_dim]
            part_ref[pl.ds(at, chunk), :] = values.astype(jnp.bfloat16)
            new = []
            for k in range(vectors):
                product = vectors_ref[k, pl.ds(at, chunk), :].astype(jnp.float32) * values
                folded = product[0:8] + product[8:16]
                pieces = [folded[:, c : c + LANE] for c in range(0, bond_dim, LANE)]
                while len(pieces) > 1:
                    pieces = [a + b for a, b in zip(pieces[0::2], pieces[1::2])]
                new.append(totals[k] + pieces[0])
            return tuple(new)

        totals = lax.fori_loop(
            0, rows // chunk, fold, tuple(jnp.zeros((8, LANE), jnp.float32) for _ in range(vectors))
        )
        for k in range(vectors):
            corr_ref[k] = totals[k]


def exchange_kernel(
    groups, sites,
    part_ref, psi_ref, left_e_ref, right_e_ref, corr_ref,
    out_ref, corr_out,
    pair_in, sending, outer_in, corr_ops, corr_sites,
    pair_s, pair_r, outer_s, outer_r, gath_s, gath_r, fwd_s, fwd_r, ops_s, ops_r, site_s, site_r,
):
    outer = groups // 2
    me = lax.axis_index("ops")
    here = lax.axis_index("site")
    row = me // 2
    side = me % 2
    peer = row * 2 + 1 - side
    rows, bond_dim = part_ref.shape[1], part_ref.shape[2]
    step = 256

    barrier = pltpu.get_barrier_semaphore()
    for k in range(1, groups):
        pl.semaphore_signal(
            barrier, inc=1, device_id={"ops": lax.rem(me + k, groups)}, device_id_type=MESH
        )
    for k in range(1, sites):
        pl.semaphore_signal(
            barrier, inc=1, device_id={"site": lax.rem(here + k, sites)}, device_id_type=MESH
        )
    pl.semaphore_wait(barrier, groups - 1 + sites - 1)

    def remote(src, dst, send_sem, recv_sem, target):
        return pltpu.make_async_remote_copy(
            src_ref=src, dst_ref=dst, send_sem=send_sem, recv_sem=recv_sem,
            device_id=target, device_id_type=MESH,
        )

    halves = 2
    width = bond_dim // halves
    parts = [pl.ds(h * width, width) for h in range(halves)]

    pair = []
    for h in range(halves):
        for k in range(outer):
            dest = lax.rem(row + k + 1, outer)
            copy = remote(
                part_ref.at[dest * 2 + 1 - side, :, parts[h]], pair_in.at[k, :, parts[h]],
                pair_s.at[h, k], pair_r.at[h, k], {"ops": peer},
            )
            copy.start()
            pair.append(copy)

    corr_copies = []
    for k in range(1, groups):
        copy = remote(
            corr_ref, corr_ops.at[k], ops_s.at[k], ops_r.at[k], {"ops": lax.rem(me + k, groups)}
        )
        copy.start()
        corr_copies.append(copy)
    corr_ops[0] = corr_ref[...]

    sends = []
    for h in range(halves):
        for k in range(outer - 1):
            dest = lax.rem(row + k + 1, outer)
            mine = dest * 2 + side
            pair[h * outer + k].wait_recv()

            def add(c, carry, k=k, mine=mine, h=h):
                cols = pl.ds(pl.multiple_of(h * width + c * step, step), step)
                sending[k, :, cols] = (
                    part_ref[mine, :, cols].astype(jnp.float32)
                    + pair_in[k, :, cols].astype(jnp.float32)
                ).astype(jnp.bfloat16)
                return carry

            lax.fori_loop(0, width // step, add, 0)
            copy = remote(
                sending.at[k, :, parts[h]], outer_in.at[k, :, parts[h]],
                outer_s.at[h, k], outer_r.at[h, k], {"ops": mine},
            )
            copy.start()
            sends.append(copy)

    gathers = []
    forwards = []
    for h in range(halves):
        pair[h * outer + outer - 1].wait_recv()
        for copy in sends[h * (outer - 1) : (h + 1) * (outer - 1)]:
            copy.wait_recv()

        def finish(c, carry, h=h):
            cols = pl.ds(pl.multiple_of(h * width + c * step, step), step)
            total = part_ref[me, :, cols].astype(jnp.float32) + pair_in[
                outer - 1, :, cols
            ].astype(jnp.float32)
            for k in range(outer - 1):
                total = total + outer_in[k, :, cols].astype(jnp.float32)
            total = total + (left_e_ref[...] + right_e_ref[:, cols]) * psi_ref[:, cols].astype(
                jnp.float32
            )
            out_ref[me, :, cols] = total.astype(jnp.bfloat16)
            return carry

        lax.fori_loop(0, width // step, finish, 0)
        block = out_ref.at[me, :, parts[h]]
        for k in range(outer - 1):
            dest = lax.rem(row + k + 1, outer)
            copy = remote(
                block, block, gath_s.at[h, k], gath_r.at[h, k], {"ops": dest * 2 + side}
            )
            copy.start()
            gathers.append(copy)
        copy = remote(
            block, block, fwd_s.at[h, outer - 1], fwd_r.at[h, outer - 1], {"ops": peer}
        )
        copy.start()
        forwards.append(copy)

    for copy in corr_copies:
        copy.wait_recv()

    def corr_add(g, total):
        return total + corr_ops[lax.rem(me - g + groups, groups)]

    corr_sites[0] = lax.fori_loop(0, groups, corr_add, jnp.zeros(corr_ref.shape, jnp.float32))
    site_copies = []
    for k in range(1, sites):
        copy = remote(
            corr_sites.at[0], corr_sites.at[k], site_s.at[k], site_r.at[k],
            {"site": lax.rem(here + k, sites)},
        )
        copy.start()
        site_copies.append(copy)

    for h in range(halves):
        for k in range(outer - 1):
            source = lax.rem(row - k - 1 + outer, outer)
            block = out_ref.at[source * 2 + side, :, parts[h]]
            remote(block, block, gath_s.at[h, k], gath_r.at[h, k], {"ops": peer}).wait_recv()
            copy = remote(block, block, fwd_s.at[h, k], fwd_r.at[h, k], {"ops": peer})
            copy.start()
            forwards.append(copy)

    for copy in site_copies:
        copy.wait_recv()

    def site_add(g, total):
        return total + corr_sites[lax.rem(here - g + sites, sites)]

    corr_out[...] = lax.fori_loop(0, sites, site_add, jnp.zeros(corr_ref.shape, jnp.float32))

    for h in range(halves):
        block = out_ref.at[peer, :, parts[h]]
        remote(
            block, block, fwd_s.at[h, outer - 1], fwd_r.at[h, outer - 1], {"ops": peer}
        ).wait_recv()
        for k in range(outer - 1):
            source = lax.rem(row - k - 1 + outer, outer)
            block = out_ref.at[source * 2 + 1 - side, :, parts[h]]
            remote(block, block, fwd_s.at[h, k], fwd_r.at[h, k], {"ops": peer}).wait_recv()
    for copy in pair + corr_copies + sends + gathers + forwards + site_copies:
        copy.wait_send()


def local(
    wavefunction,
    left_blocks,
    right_blocks,
    left_sector,
    right_sector,
    term_count,
    left_energy,
    right_energy,
    subspace,
):
    slots, sec_dev, widest = left_blocks.shape[0], left_blocks.shape[1], left_blocks.shape[2]
    bond_dim = wavefunction.shape[0]
    vectors = subspace.shape[0]
    rows = sec_dev * widest
    sites = lax.axis_size("site")
    groups = lax.axis_size("ops")
    sectors = sec_dev * sites
    wide = round_up(widest, 256)
    window = round_up(widest + LANE - 1, LANE)
    padded_cols = round_up(bond_dim, LANE) - LANE + window

    assert sites == 4 and slots % 2 == 0 and 2 * (wide - widest) == LANE and wide == 2 * LANE
    right = right_blocks.transpose(1, 2, 0, 3).reshape(sec_dev, widest, slots * widest)

    left_start, left_size = sector_tables(left_sector, sectors)
    right_start, right_size = sector_tables(right_sector, sectors)
    first_sector = lax.axis_index("site") * sec_dev
    psi_padded = jnp.pad(wavefunction, ((0, widest), (0, padded_cols - bond_dim)))
    energy_padded = jnp.pad(left_energy, (0, widest))
    slabs = []
    energies = []
    insides = []
    for within in range(sec_dev):
        row_start = left_start[first_sector + within]
        inside = jnp.arange(widest, dtype=jnp.int32) < left_size[first_sector + within]
        slab = lax.dynamic_slice_in_dim(psi_padded, row_start, widest, 0)
        slabs.append(jnp.where(inside[:, None], slab, jnp.zeros((), slab.dtype)))
        energies.append(lax.dynamic_slice_in_dim(energy_padded, row_start, widest, 0))
        insides.append(inside)
    slab = jnp.concatenate(slabs, axis=0)
    energy = jnp.concatenate(energies)
    inside = jnp.stack(insides)
    live = jnp.arange(slots, dtype=jnp.int32) < term_count[0]
    keep = live[:, None, None, None] & inside[None, :, :, None] & inside[None, :, None, :]
    left = jnp.where(keep, left_blocks, jnp.zeros((), left_blocks.dtype))
    left = left.reshape(slots // 2, 2, sec_dev, widest, widest).transpose(2, 1, 0, 3, 4)
    left = left.reshape(sec_dev, 2, slots // 2 * widest, widest)
    vectors_flat = subspace.reshape(vectors, rows, bond_dim)

    own = lax.axis_index("ops")
    psi_mine = slab[:, :bond_dim]
    diagonal = (energy[:, None] + right_energy[None, :]) * psi_mine.astype(jnp.float32)
    first_group = jnp.where(own == 0, jnp.float32(1.0), jnp.float32(0.0))
    corr_diag = first_group * jnp.sum(
        vectors_flat.astype(jnp.float32) * diagonal[None], axis=(1, 2)
    )

    vmem = pl.BlockSpec(memory_space=pltpu.VMEM)
    smem = pl.BlockSpec(memory_space=pltpu.SMEM)
    dma = pltpu.SemaphoreType.DMA
    spread = pl.pallas_call(
        functools.partial(spread_kernel, wide, window),
        grid=(sectors,),
        out_shape=jax.ShapeDtypeStruct((sectors, rows, wide), jnp.bfloat16),
        in_specs=[smem, smem, vmem],
        out_specs=pl.BlockSpec((1, rows, wide), lambda step: (step, 0, 0)),
        compiler_params=pltpu.CompilerParams(
            dimension_semantics=("arbitrary",), vmem_limit_bytes=40 * 1024 * 1024
        ),
        name="spread_columns",
    )(right_start, right_size, slab)
    added = pl.pallas_call(
        functools.partial(apply_kernel, slots, sec_dev, widest, wide),
        out_shape=jax.ShapeDtypeStruct((sectors, rows, wide), jnp.float32),
        in_specs=[vmem, vmem, vmem],
        out_specs=pl.BlockSpec(memory_space=pl.ANY),
        scratch_shapes=[
            pltpu.VMEM((2, rows, wide), jnp.bfloat16),
            pltpu.VMEM((rows, slots * widest), jnp.bfloat16),
            pltpu.VMEM((wide, slots * widest), jnp.bfloat16),
            pltpu.VMEM((3, sec_dev, widest, slots * widest), jnp.bfloat16),
            pltpu.VMEM((2, rows, wide), jnp.float32),
            dma((sec_dev,)), dma((sec_dev,)),
            dma((sec_dev,)), dma((sec_dev,)),
            dma((sec_dev,)), dma((sec_dev,)),
            dma((2,)),
        ],
        compiler_params=pltpu.CompilerParams(
            collective_id=1, has_side_effects=True, vmem_limit_bytes=60 * 1024 * 1024
        ),
        name="apply_terms",
    )(left, spread, right)
    part, corr = pl.pallas_call(
        functools.partial(place_kernel, widest, wide, window),
        grid=(sectors,),
        out_shape=(
            jax.ShapeDtypeStruct((rows, bond_dim), jnp.bfloat16),
            jax.ShapeDtypeStruct((vectors, 8, LANE), jnp.float32),
        ),
        in_specs=[smem, smem, pl.BlockSpec((1, rows, wide), lambda step: (step, 0, 0)), vmem],
        out_specs=(vmem, vmem),
        scratch_shapes=[pltpu.VMEM((rows, padded_cols), jnp.float32)],
        compiler_params=pltpu.CompilerParams(
            dimension_semantics=("arbitrary",), vmem_limit_bytes=60 * 1024 * 1024
        ),
        name="place_columns",
    )(right_start, right_size, added, vectors_flat)

    share = rows // groups
    corr_mine = jnp.sum(corr, axis=(1, 2)) + corr_diag
    corr_tile = jnp.broadcast_to(corr_mine[:, None, None], (vectors, 8, LANE))
    psi_share = lax.dynamic_slice_in_dim(psi_mine, own * share, share, 0)
    energy_share = lax.dynamic_slice_in_dim(energy, own * share, share, 0)[:, None]
    outer = groups // 2
    sigma, corr_all = pl.pallas_call(
        functools.partial(exchange_kernel, groups, sites),
        out_shape=(
            jax.ShapeDtypeStruct((groups, share, bond_dim), jnp.bfloat16),
            jax.ShapeDtypeStruct((vectors, 8, LANE), jnp.float32),
        ),
        in_specs=[vmem] * 5,
        out_specs=(vmem, vmem),
        scratch_shapes=[
            pltpu.VMEM((outer, share, bond_dim), jnp.bfloat16),
            pltpu.VMEM((max(outer - 1, 1), share, bond_dim), jnp.bfloat16),
            pltpu.VMEM((max(outer - 1, 1), share, bond_dim), jnp.bfloat16),
            pltpu.VMEM((groups, vectors, 8, LANE), jnp.float32),
            pltpu.VMEM((sites, vectors, 8, LANE), jnp.float32),
            dma((2, outer)), dma((2, outer)),
            dma((2, outer)), dma((2, outer)),
            dma((2, outer)), dma((2, outer)),
            dma((2, outer)), dma((2, outer)),
            dma((groups,)), dma((groups,)),
            dma((sites,)), dma((sites,)),
        ],
        compiler_params=pltpu.CompilerParams(
            collective_id=0, has_side_effects=True, vmem_limit_bytes=60 * 1024 * 1024
        ),
        name="exchange_rows",
    )(
        part.reshape(groups, share, bond_dim),
        psi_share,
        energy_share,
        right_energy[None, :],
        corr_tile,
    )
    return (sigma.reshape(sec_dev, widest, bond_dim), corr_all[:, 0, 0])


def solution(mesh):
    in_specs = (
        P(),
        P("ops", "site", None, None),
        P("ops", "site", None, None),
        P(),
        P(),
        P("ops"),
        P(),
        P(),
        P(None, "site", None, None),
    )
    out_specs = (P("site", None, None), P())
    return jax.shard_map(local, mesh=mesh, in_specs=in_specs, out_specs=out_specs, check_vma=False)
```
